128 devices in a mesh: owner: 4 (over y_lo, core), rows: 32 (over z, y_hi, x).
Axes of the slice: x: 4, y: 4 (y_hi: 2, y_lo: 2; y = y_hi * 2 + y_lo), z: 4, core: 2. Of those that a mesh axis runs over, the one named last changes fastest.
Arguments:
- train_gate: float32 [128, 2048, 768], P('owner', 'rows'), may hold values from -0.125 to 0.125
- train_up: float32 [128, 2048, 768], P('owner', 'rows'), may hold values from -0.125 to 0.125
- router_weight: float32 [2048, 128], P('rows', 'owner'), may hold values from -0.125 to 0.125
- router_gain: float32 [2048], P('rows'), may hold values from 0.25 to 1.75
Outputs:
- ready_gate: bfloat16 [128, 768, 2048], P(('owner', 'rows'))
- ready_up: bfloat16 [128, 768, 2048], P(('owner', 'rows'))
- serve_router: bfloat16 [2048, 128], replicated
The draws below stay inside these ranges and needn't reach their ends.
All inputs are finite; a program needn't handle non-finite values.
Results may differ from the reference program's by a relative error of at most 0.001.
Values may be sent and summed in bfloat16 or wider, within the bound.
No kernel may reach another device: no remote copies, remote signals or barrier semaphores. Data moves between devices by JAX's collectives and lax.ppermute only.
A program may use at most 128 MiB of HBM per device.

```python
import jax
import jax.numpy as jnp

EXPERTS = 128
D_MODEL = 2048
D_EXPERT = 768


def level_of(stream_key, extent, pieces, smallest, top_value):
    level, own = 1.0, jax.random.fold_in(stream_key, 6)
    for position, parts in pieces:
        draws = jnp.exp(jax.random.uniform(jax.random.fold_in(own, position), (parts,), jnp.float32, smallest / len(pieces), top_value / len(pieces)))
        level = level * jnp.repeat(draws, extent[position] // parts).reshape([-1 if axis == position else 1 for axis in range(len(extent))])
    return level


def normal_values(key, shape, deviation, limit, cuts=(), held_as=jnp.bfloat16):
    entries = deviation * jax.random.normal(key, shape, jnp.float32)
    if cuts:
        entries = entries * level_of(key, shape, cuts, -0.22, 0.18)
    return jnp.clip(entries, -limit, limit).astype(held_as)


def setup_inputs(seed: int = 0) -> dict:
    arg_keys = jax.random.split(jax.random.key(seed), 5)
    return {
        "train_gate": normal_values(arg_keys[0], (EXPERTS, D_MODEL, D_EXPERT), D_MODEL ** -0.5, 0.125, ((0, 4), (1, 32)), jnp.float32),
        "train_up": normal_values(arg_keys[1], (EXPERTS, D_MODEL, D_EXPERT), D_MODEL ** -0.5, 0.125, ((0, 4), (1, 32)), jnp.float32),
        "router_weight": normal_values(arg_keys[2], (D_MODEL, EXPERTS), D_MODEL ** -0.5, 0.125, ((0, 32), (1, 4)), jnp.float32),
        "router_gain": jnp.clip(1.0 + 0.15 * jax.random.normal(arg_keys[3], (D_MODEL,), jnp.float32), 0.25, 1.75),
    }


def reference(train_gate, train_up, router_weight, router_gain):
    ready_gate = train_gate.astype(jnp.bfloat16)
    ready_gate = jnp.transpose(ready_gate, (0, 2, 1))
    ready_up = train_up.astype(jnp.bfloat16)
    ready_up = jnp.transpose(ready_up, (0, 2, 1))
    serve_router = (router_weight * router_gain[:, None]).astype(jnp.bfloat16)
    return ready_gate, ready_up, serve_router
```

```python
import jax
import jax.numpy as jnp
from jax import lax
from jax.sharding import PartitionSpec as P


def on_device(train_gate, train_up, router_weight, router_gain):
    narrow_gate, narrow_up = (train_gate.astype(jnp.bfloat16), train_up.astype(jnp.bfloat16))
    ready_gate, ready_up = (
        lax.all_to_all(narrow_gate, "rows", split_axis=0, concat_axis=1, tiled=True),
        lax.all_to_all(narrow_up, "rows", split_axis=0, concat_axis=1, tiled=True),
    )
    ready_gate = jnp.transpose(ready_gate, (0, 2, 1))
    ready_up = jnp.transpose(ready_up, (0, 2, 1))
    part_router = (router_weight * router_gain[:, None]).astype(jnp.bfloat16)
    row_router = lax.all_gather(part_router, "rows", axis=0, tiled=True)
    serve_router = lax.all_gather(row_router, "owner", axis=1, tiled=True)
    return (ready_gate, ready_up, serve_router)


def solution(mesh):
    placed = (P("owner", "rows", None), P("owner", "rows", None), P("rows", "owner"), P("rows"))
    return jax.shard_map(
        on_device,
        mesh=mesh,
        in_specs=placed,
        out_specs=(P(("owner", "rows"), None, None), P(("owner", "rows"), None, None), P()),
        check_vma=False,
    )
```

```python
import jax
import jax.numpy as jnp
from jax import lax
from jax.experimental import pallas as pl
from jax.experimental.pallas import tpu as pltpu
from jax.sharding import PartitionSpec as P

AXES = ("owner", "rows")
LANES = 128
WHOLE = pl.BlockSpec(memory_space=pltpu.VMEM)
COST = pl.CostEstimate(flops=100_000_000, bytes_accessed=20_000_000, transcendentals=0)


def places():
    for owner in range(4):
        for row in range(32):
            yield {"z": row // 8, "yh": row // 4 % 2, "x": row % 4, "yl": owner // 2, "core": owner % 2}


def place(at):
    return (at["yl"] * 2 + at["core"]) * 32 + at["z"] * 8 + at["yh"] * 4 + at["x"]


def swap(block, axis):
    pairs = [(place(at), place(dict(at, **{axis: at[axis] ^ 1}))) for at in places()]
    return lax.ppermute(block, AXES, pairs)


def pack_kernel(gate_ref, up_ref, out_ref, held, sems):
    deep, wide = gate_ref.shape[1:]
    step, batches = held.shape[2], held.shape[1]
    tiles = wide // LANES

    def copy(which, ref, batch):
        return pltpu.make_async_copy(
            ref.at[pl.ds(batch * step, step)], held.at[which, batch], sems.at[which, batch]
        )

    for batch in range(batches):
        for which, ref in enumerate((gate_ref, up_ref)):
            copy(which, ref, batch).start()

    def convert(batch, carry):
        for which, ref in enumerate((gate_ref, up_ref)):
            copy(which, ref, batch).wait()
            for tile in range(tiles):
                out_ref[pl.ds(batch * step, step), pl.ds((which * tiles + tile) * deep, deep), :] = held[
                    which, batch, :, :, tile * LANES : (tile + 1) * LANES
                ].astype(jnp.bfloat16)
        return carry

    lax.fori_loop(0, batches, convert, 0)


def pack(gate, up, extra):
    pieces, deep, wide = gate.shape
    step = 2
    total = 2 * deep * wide // LANES + extra
    anywhere = pl.BlockSpec(memory_space=pltpu.HBM)
    return pl.pallas_call(
        pack_kernel,
        in_specs=[anywhere, anywhere],
        out_specs=WHOLE,
        out_shape=pltpu.VMEM((pieces, total, LANES), jnp.bfloat16),
        scratch_shapes=[
            pltpu.VMEM((2, pieces // step, step, deep, wide), jnp.float32),
            pltpu.SemaphoreType.DMA((2, pieces // step)),
        ],
        compiler_params=pltpu.CompilerParams(vmem_limit_bytes=44 * 1024 * 1024),
        cost_estimate=COST,
        name="pack",
    )(gate, up)


def stamp_kernel(payload_ref, mine_ref, other_ref, out_ref):
    del payload_ref
    upper = lax.axis_index("owner") // 2 == 1
    mine, other = mine_ref[...].astype(jnp.float32), other_ref[...].astype(jnp.float32)
    both = jnp.concatenate([jnp.where(upper, other, mine), jnp.where(upper, mine, other)], axis=0).T
    deep = both.shape[0]
    block = jnp.concatenate([both[: deep // 2], both[deep // 2 :]], axis=1).astype(jnp.bfloat16)
    first = out_ref.shape[1] - deep // 2
    for piece in range(out_ref.shape[0]):
        out_ref[piece, first:, :] = block


def stamp(payload, mine, other):
    return pl.pallas_call(
        stamp_kernel,
        in_specs=[WHOLE, WHOLE, WHOLE],
        out_specs=WHOLE,
        out_shape=jax.ShapeDtypeStruct(payload.shape, payload.dtype),
        input_output_aliases={0: 0},
        compiler_params=pltpu.CompilerParams(vmem_limit_bytes=16 * 1024 * 1024),
        name="stamp",
    )(payload, mine, other)


def unpack_kernel(source, gate_ref, up_ref):
    pieces = source.shape[0]
    deep = gate_ref.shape[1] // pieces
    tiles = pl.num_programs(0)
    pair = LANES // deep
    for which, out in enumerate((gate_ref, up_ref)):
        start = (which * tiles + pl.program_id(0)) * deep
        for i in range(pieces // pair):
            block = source[pl.ds(i * pair, pair), pl.ds(pl.multiple_of(start, deep), deep), :]
            out[:, i * LANES : (i + 1) * LANES] = block.reshape(LANES, LANES).T


def unpack(received, deep, wide):
    pieces = received.shape[0]
    out = pl.BlockSpec((LANES, pieces * deep), lambda j: (j, 0))
    shape = jax.ShapeDtypeStruct((wide, pieces * deep), jnp.bfloat16)
    return pl.pallas_call(
        unpack_kernel,
        grid=(wide // LANES,),
        in_specs=[WHOLE],
        out_specs=[out, out],
        out_shape=[shape, shape],
        compiler_params=pltpu.CompilerParams(vmem_limit_bytes=16 * 1024 * 1024),
        cost_estimate=COST,
        name="unpack",
    )(received)


def finish_kernel(mine_ref, other_ref, out_ref):
    pieces, half, lanes = mine_ref.shape
    upper = lax.axis_index("owner") % 2 == 1
    mine = mine_ref[...].reshape(pieces * half, lanes).astype(jnp.float32)
    other = other_ref[...].reshape(pieces * half, lanes).astype(jnp.float32)
    first, second = jnp.where(upper, other, mine), jnp.where(upper, mine, other)
    quarter = lanes // 4
    group = lax.broadcasted_iota(jnp.int32, first.shape, 1) // quarter
    for h in range(2):
        parts = [
            pltpu.roll(first, (lanes - 2 * quarter * h) % lanes, 1),
            pltpu.roll(second, (lanes + quarter - 2 * quarter * h) % lanes, 1),
            pltpu.roll(first, (lanes + quarter - 2 * quarter * h) % lanes, 1),
            pltpu.roll(second, (lanes + 2 * quarter - 2 * quarter * h) % lanes, 1),
        ]
        block = parts[3]
        for i in range(3):
            block = jnp.where(group == i, parts[i], block)
        out_ref[:, h * half : (h + 1) * half, :] = block.astype(jnp.bfloat16).reshape(pieces, half, lanes)


def finish(mine, other):
    pieces, half, lanes = mine.shape
    return pl.pallas_call(
        finish_kernel,
        in_specs=[WHOLE, WHOLE],
        out_specs=WHOLE,
        out_shape=jax.ShapeDtypeStruct((pieces, 2 * half, lanes), jnp.bfloat16),
        compiler_params=pltpu.CompilerParams(vmem_limit_bytes=8 * 1024 * 1024),
        name="finish",
    )(mine, other)


def on_device(train_gate, train_up, router_weight, router_gain):
    pieces, deep, wide = train_gate.shape
    part = (router_weight.T * router_gain[None, :]).astype(jnp.bfloat16)
    part = lax.optimization_barrier(part)
    other_part = swap(part, "yl")
    payload = pack(train_gate, train_up, deep // 2)
    body = payload.shape[1] - deep // 2
    payload = stamp(payload, part, other_part)
    received = lax.all_to_all(payload, "rows", split_axis=0, concat_axis=0, tiled=True)
    mine = received[:, body:, :]
    other = swap(mine, "core")
    ready_gate, ready_up = unpack(received, deep, wide)
    serve_router = finish(mine, other).reshape(pieces * deep, LANES)
    return (ready_gate[None], ready_up[None], serve_router)


def solution(mesh):
    placed = (P("owner", "rows", None), P("owner", "rows", None), P("rows", "owner"), P("rows"))
    return jax.shard_map(
        on_device,
        mesh=mesh,
        in_specs=placed,
        out_specs=(P(("owner", "rows"), None, None), P(("owner", "rows"), None, None), P()),
        check_vma=False,
    )
```

```python
import jax
import jax.numpy as jnp
from jax import lax
from jax.experimental import pallas as pl
from jax.experimental.pallas import tpu as pltpu
from jax.sharding import PartitionSpec as P

AXES = ("owner", "rows")
LANES = 128
WHOLE = pl.BlockSpec(memory_space=pltpu.VMEM)
COST = pl.CostEstimate(flops=100_000_000, bytes_accessed=20_000_000, transcendentals=0)


def places():
    for owner in range(4):
        for row in range(32):
            yield {"z": row // 8, "yh": row // 4 % 2, "x": row % 4, "yl": owner // 2, "core": owner % 2}


def place(at):
    return (at["yl"] * 2 + at["core"]) * 32 + at["z"] * 8 + at["yh"] * 4 + at["x"]


def swap(block, axis):
    pairs = [(place(at), place(dict(at, **{axis: at[axis] ^ 1}))) for at in places()]
    return lax.ppermute(block, AXES, pairs)


def pack_kernel(gate_ref, up_ref, out_ref, held, sems):
    batches, step, deep, wide = held.shape[1:]
    tiles = wide // LANES

    def copy(which, batch):
        source = (gate_ref, up_ref)[which]
        return pltpu.make_async_copy(source.at[pl.ds(batch * step, step)], held.at[which, batch], sems.at[which, batch])

    for batch in range(batches):
        for which in range(2):
            copy(which, batch).start()

    @pl.loop(0, batches)
    def _(batch):
        for which in range(2):
            copy(which, batch).wait()
            for tile in range(tiles):
                out_ref[pl.ds(batch * step, step), pl.ds((which * tiles + tile) * deep, deep), :] = held[
                    which, batch, :, :, tile * LANES : (tile + 1) * LANES
                ].astype(jnp.bfloat16)


def pack(gate, up, extra):
    pieces, deep, wide = gate.shape
    step = 4
    total = 2 * deep * wide // LANES + extra
    there = pl.BlockSpec(memory_space=pltpu.HBM)
    return pl.pallas_call(
        pack_kernel,
        in_specs=[there, there],
        out_specs=WHOLE,
        out_shape=pltpu.VMEM((pieces, total, LANES), jnp.bfloat16),
        scratch_shapes=[
            pltpu.VMEM((2, pieces // step, step, deep, wide), jnp.float32),
            pltpu.SemaphoreType.DMA((2, pieces // step)),
        ],
        compiler_params=pltpu.CompilerParams(vmem_limit_bytes=44 * 1024 * 1024),
        cost_estimate=COST,
        name="pack",
    )(gate, up)


def stamp_kernel(payload_ref, mine_ref, other_ref, gain_ref, out_ref):
    del payload_ref
    upper = lax.axis_index("owner") // 2 == 1
    mine, other = mine_ref[...] * gain_ref[...], other_ref[...] * gain_ref[...]
    both = jnp.concatenate([jnp.where(upper, other, mine), jnp.where(upper, mine, other)], axis=0).T
    half, width = both.shape[0] // 2, both.shape[1] // 2
    parts = [both[h * half : (h + 1) * half, w * width : (w + 1) * width] for w in range(2) for h in range(2)]
    swapped = jnp.concatenate([parts[i ^ 1] for i in range(4)], axis=1)
    block = jnp.where(lax.axis_index("owner") % 2 == 1, swapped, jnp.concatenate(parts, axis=1))
    block = block.astype(jnp.bfloat16)
    first = out_ref.shape[1] - half
    for piece in range(out_ref.shape[0]):
        out_ref[piece, first:, :] = block


def stamp(payload, mine, other, gain):
    return pl.pallas_call(
        stamp_kernel,
        in_specs=[WHOLE] * 4,
        out_specs=WHOLE,
        out_shape=jax.ShapeDtypeStruct(payload.shape, payload.dtype),
        input_output_aliases={0: 0},
        compiler_params=pltpu.CompilerParams(vmem_limit_bytes=16 * 1024 * 1024),
        name="stamp",
    )(payload, mine, other, gain)


def unpack_kernel(source, gate_ref, up_ref, held, sems):
    pieces = source.shape[0]
    deep = gate_ref.shape[1] // pieces
    tiles = held.shape[1]
    pair = LANES // deep

    def copy(which, tile):
        out = (gate_ref, up_ref)[which]
        return pltpu.make_async_copy(held.at[which, tile], out.at[pl.ds(tile * LANES, LANES)], sems.at[which, tile])

    @pl.loop(0, tiles)
    def _(tile):
        for which in range(2):
            start = pl.multiple_of((which * tiles + tile) * deep, deep)
            for i in range(pieces // pair):
                block = source[pl.ds(i * pair, pair), pl.ds(start, deep), :]
                held[which, tile, :, i * LANES : (i + 1) * LANES] = block.reshape(LANES, LANES).T
            copy(which, tile).start()

    @pl.loop(0, tiles)
    def _(tile):
        for which in range(2):
            copy(which, tile).wait()


def unpack(received, deep, wide):
    pieces = received.shape[0]
    there = pl.BlockSpec(memory_space=pltpu.HBM)
    shape = jax.ShapeDtypeStruct((wide, pieces * deep), jnp.bfloat16)
    return pl.pallas_call(
        unpack_kernel,
        in_specs=[WHOLE],
        out_specs=[there, there],
        out_shape=[shape, shape],
        scratch_shapes=[
            pltpu.VMEM((2, wide // LANES, LANES, pieces * deep), jnp.bfloat16),
            pltpu.SemaphoreType.DMA((2, wide // LANES)),
        ],
        compiler_params=pltpu.CompilerParams(vmem_limit_bytes=24 * 1024 * 1024),
        cost_estimate=COST,
        name="unpack",
    )(received)


def finish_kernel(mine_ref, other_ref, out_ref):
    pieces, half, lanes = mine_ref.shape
    upper = lax.axis_index("owner") % 2
    mine = mine_ref[...].reshape(pieces * half, lanes).astype(jnp.float32)
    other = other_ref[...].reshape(pieces * half, lanes).astype(jnp.float32)
    quarter = lanes // 4
    odd = lax.broadcasted_iota(jnp.int32, mine.shape, 1) // quarter % 2
    own = odd == upper
    crossed = jnp.where(own, other, mine)
    crossed = jnp.where(odd == 1, pltpu.roll(crossed, quarter, 1), pltpu.roll(crossed, lanes - quarter, 1))
    for h, block in enumerate((jnp.where(own, mine, other), crossed)):
        out_ref[:, h * half : (h + 1) * half, :] = block.astype(jnp.bfloat16).reshape(pieces, half, lanes)


def finish(mine, other):
    pieces, half, lanes = mine.shape
    return pl.pallas_call(
        finish_kernel,
        in_specs=[WHOLE, WHOLE],
        out_specs=WHOLE,
        out_shape=jax.ShapeDtypeStruct((pieces, 2 * half, lanes), jnp.bfloat16),
        compiler_params=pltpu.CompilerParams(vmem_limit_bytes=8 * 1024 * 1024),
        name="finish",
    )(mine, other)


def on_device(train_gate, train_up, router_weight, router_gain):
    pieces, deep, wide = train_gate.shape
    part = router_weight.T
    other_part = swap(part, "yl")
    payload = pack(train_gate, train_up, deep // 2)
    body = payload.shape[1] - deep // 2
    payload = stamp(payload, part, other_part, router_gain[None, :])
    received = lax.all_to_all(payload, "rows", split_axis=0, concat_axis=0, tiled=True)
    mine = received[:, body:, :]
    other = swap(mine, "core")
    ready_gate, ready_up = unpack(received, deep, wide)
    serve_router = finish(mine, other).reshape(pieces * deep, LANES)
    return (ready_gate[None], ready_up[None], serve_router)


def solution(mesh):
    placed = (P("owner", "rows", None), P("owner", "rows", None), P("rows", "owner"), P("rows"))
    return jax.shard_map(
        on_device,
        mesh=mesh,
        in_specs=placed,
        out_specs=(P(("owner", "rows"), None, None), P(("owner", "rows"), None, None), P()),
        check_vma=False,
    )
```

```python
import jax
import jax.numpy as jnp
from jax import lax
from jax.experimental import pallas as pl
from jax.experimental.pallas import tpu as pltpu
from jax.sharding import PartitionSpec as P

AXES = ("owner", "rows")
LANES = 128
MEMBERS = [(3 - z) * 8 + (1 - yh) * 4 + (3 - x) for z in range(4) for yh in range(2) for x in range(4)]
SLOT = [MEMBERS.index(row) for row in range(32)]
WHOLE = pl.BlockSpec(memory_space=pltpu.VMEM)
COST = pl.CostEstimate(flops=100_000_000, bytes_accessed=20_000_000, transcendentals=0)


def places():
    for owner in range(4):
        for row in range(32):
            yield {"z": row // 8, "yh": row // 4 % 2, "x": row % 4, "yl": owner // 2, "core": owner % 2}


def place(at):
    return (at["yl"] * 2 + at["core"]) * 32 + at["z"] * 8 + at["yh"] * 4 + at["x"]


def swap(block, axis):
    pairs = [(place(at), place(dict(at, **{axis: at[axis] ^ 1}))) for at in places()]
    return lax.ppermute(block, AXES, pairs)


def pack_kernel(gate_ref, up_ref, out_ref, held, sems):
    batches, step, deep, wide = held.shape[1:]
    tiles = wide // LANES

    def copy(which, batch):
        source = (gate_ref, up_ref)[which]
        return pltpu.make_async_copy(source.at[pl.ds(batch * step, step)], held.at[which, batch], sems.at[which, batch])

    for batch in range(batches):
        for which in range(2):
            copy(which, batch).start()

    for batch in range(batches):
        for which in range(2):
            copy(which, batch).wait()
            for piece in range(step):
                slot = SLOT[batch * step + piece]

                @pl.loop(0, tiles)
                def _(tile):
                    first = pl.multiple_of((which * tiles + tile) * deep, deep)
                    lanes = pl.ds(pl.multiple_of(tile * LANES, LANES), LANES)
                    out_ref[slot, pl.ds(first, deep), :] = held[which, batch, piece, :, lanes].astype(jnp.bfloat16)


def pack(gate, up, extra):
    pieces, deep, wide = gate.shape
    step = 4
    total = 2 * deep * wide // LANES + extra
    there = pl.BlockSpec(memory_space=pltpu.HBM)
    return pl.pallas_call(
        pack_kernel,
        in_specs=[there, there],
        out_specs=WHOLE,
        out_shape=pltpu.VMEM((pieces, total, LANES), jnp.bfloat16),
        scratch_shapes=[
            pltpu.VMEM((2, pieces // step, step, deep, wide), jnp.float32),
            pltpu.SemaphoreType.DMA((2, pieces // step)),
        ],
        compiler_params=pltpu.CompilerParams(vmem_limit_bytes=44 * 1024 * 1024),
        cost_estimate=COST,
        name="pack",
    )(gate, up)


def stamp_kernel(payload_ref, mine_ref, other_ref, gain_ref, out_ref):
    del payload_ref
    upper = lax.axis_index("owner") // 2 == 1
    mine, other = mine_ref[...] * gain_ref[...], other_ref[...] * gain_ref[...]
    both = jnp.concatenate([jnp.where(upper, other, mine), jnp.where(upper, mine, other)], axis=0).T
    half, width = both.shape[0] // 2, both.shape[1] // 2
    parts = [both[h * half : (h + 1) * half, w * width : (w + 1) * width] for w in range(2) for h in range(2)]
    swapped = jnp.concatenate([parts[i ^ 1] for i in range(4)], axis=1)
    block = jnp.where(lax.axis_index("owner") % 2 == 1, swapped, jnp.concatenate(parts, axis=1))
    block = block.astype(jnp.bfloat16)
    first = out_ref.shape[1] - half
    for piece in range(out_ref.shape[0]):
        out_ref[piece, first:, :] = block


def stamp(payload, mine, other, gain):
    return pl.pallas_call(
        stamp_kernel,
        in_specs=[WHOLE] * 4,
        out_specs=WHOLE,
        out_shape=jax.ShapeDtypeStruct(payload.shape, payload.dtype),
        input_output_aliases={0: 0},
        compiler_params=pltpu.CompilerParams(vmem_limit_bytes=16 * 1024 * 1024),
        name="stamp",
    )(payload, mine, other, gain)


def unpack_kernel(source, gate_ref, up_ref, held, sems):
    pieces = source.shape[0]
    deep = gate_ref.shape[1] // pieces
    tiles = held.shape[1]
    pair = LANES // deep

    def copy(which, tile):
        out = (gate_ref, up_ref)[which]
        return pltpu.make_async_copy(held.at[which, tile], out.at[pl.ds(tile * LANES, LANES)], sems.at[which, tile])

    @pl.loop(0, tiles)
    def _(tile):
        for which in range(2):
            start = pl.multiple_of((which * tiles + tile) * deep, deep)
            for i in range(pieces // pair):
                parts = [source[SLOT[i * pair + part], pl.ds(start, deep), :] for part in range(pair)]
                held[which, tile, :, i * LANES : (i + 1) * LANES] = jnp.concatenate(parts, axis=0).T
            copy(which, tile).start()

    @pl.loop(0, tiles)
    def _(tile):
        for which in range(2):
            copy(which, tile).wait()


def unpack(received, deep, wide):
    pieces = received.shape[0]
    there = pl.BlockSpec(memory_space=pltpu.HBM)
    shape = jax.ShapeDtypeStruct((wide, pieces * deep), jnp.bfloat16)
    return pl.pallas_call(
        unpack_kernel,
        in_specs=[WHOLE],
        out_specs=[there, there],
        out_shape=[shape, shape],
        scratch_shapes=[
            pltpu.VMEM((2, wide // LANES, LANES, pieces * deep), jnp.bfloat16),
            pltpu.SemaphoreType.DMA((2, wide // LANES)),
        ],
        compiler_params=pltpu.CompilerParams(vmem_limit_bytes=24 * 1024 * 1024),
        cost_estimate=COST,
        name="unpack",
    )(received)


def finish_kernel(mine_ref, other_ref, out_ref):
    pieces, half, lanes = mine_ref.shape
    upper = lax.axis_index("owner") % 2
    mine = mine_ref[...].reshape(pieces * half, lanes).astype(jnp.float32)
    other = other_ref[...].reshape(pieces * half, lanes).astype(jnp.float32)
    quarter = lanes // 4
    odd = lax.broadcasted_iota(jnp.int32, mine.shape, 1) // quarter % 2
    own = odd == upper
    crossed = jnp.where(own, other, mine)
    crossed = jnp.where(odd == 1, pltpu.roll(crossed, quarter, 1), pltpu.roll(crossed, lanes - quarter, 1))
    for h, block in enumerate((jnp.where(own, mine, other), crossed)):
        block = block.astype(jnp.bfloat16).reshape(pieces, half, lanes)
        for row in range(pieces):
            out_ref[row, h * half : (h + 1) * half, :] = block[SLOT[row]]


def finish(mine, other):
    pieces, half, lanes = mine.shape
    return pl.pallas_call(
        finish_kernel,
        in_specs=[WHOLE, WHOLE],
        out_specs=WHOLE,
        out_shape=jax.ShapeDtypeStruct((pieces, 2 * half, lanes), jnp.bfloat16),
        compiler_params=pltpu.CompilerParams(vmem_limit_bytes=8 * 1024 * 1024),
        name="finish",
    )(mine, other)


def on_device(train_gate, train_up, router_weight, router_gain):
    pieces, deep, wide = train_gate.shape
    part = router_weight.T
    other_part = swap(part, "yl")
    payload = pack(train_gate, train_up, deep // 2)
    body = payload.shape[1] - deep // 2
    payload = stamp(payload, part, other_part, router_gain[None, :])
    received = lax.all_to_all(
        payload, "rows", split_axis=0, concat_axis=0, axis_index_groups=[MEMBERS], tiled=True
    )
    mine = received[:, body:, :]
    other = swap(mine, "core")
    ready_gate, ready_up = unpack(received, deep, wide)
    serve_router = finish(mine, other).reshape(pieces * deep, LANES)
    return (ready_gate[None], ready_up[None], serve_router)


def solution(mesh):
    placed = (P("owner", "rows", None), P("owner", "rows", None), P("rows", "owner"), P("rows"))
    return jax.shard_map(
        on_device,
        mesh=mesh,
        in_specs=placed,
        out_specs=(P(("owner", "rows"), None, None), P(("owner", "rows"), None, None), P()),
        check_vma=False,
    )
```

```python
import jax
import jax.numpy as jnp
from jax import lax
from jax.experimental import pallas as pl
from jax.experimental.pallas import tpu as pltpu
from jax.sharding import PartitionSpec as P

AXES = ("owner", "rows")
LANES = 128
MEMBERS = [z * 8 + yh * 4 + x for z in (2, 3, 0, 1) for yh in (1, 0) for x in (3, 2, 1, 0)]
SLOT = [MEMBERS.index(row) for row in range(32)]
WHOLE = pl.BlockSpec(memory_space=pltpu.VMEM)
COST = pl.CostEstimate(flops=100_000_000, bytes_accessed=20_000_000, transcendentals=0)


def places():
    for owner in range(4):
        for row in range(32):
            yield {"z": row // 8, "yh": row // 4 % 2, "x": row % 4, "yl": owner // 2, "core": owner % 2}


def place(at):
    return (at["yl"] * 2 + at["core"]) * 32 + at["z"] * 8 + at["yh"] * 4 + at["x"]


def swap(block, axis):
    pairs = [(place(at), place(dict(at, **{axis: at[axis] ^ 1}))) for at in places()]
    return lax.ppermute(block, AXES, pairs)


def pack_kernel(gate_ref, up_ref, out_ref, held, sems):
    batches, step, deep, wide = held.shape[1:]
    tiles = wide // LANES

    def copy(which, batch):
        source = (gate_ref, up_ref)[which]
        return pltpu.make_async_copy(source.at[pl.ds(batch * step, step)], held.at[which, batch], sems.at[which, batch])

    for batch in range(batches):
        for which in range(2):
            copy(which, batch).start()

    for batch in range(batches):
        for which in range(2):
            copy(which, batch).wait()
            for piece in range(step):
                slot = SLOT[batch * step + piece]
                for tile in range(tiles):
                    first = (which * tiles + tile) * deep
                    out_ref[slot, first : first + deep, :] = held[
                        which, batch, piece, :, tile * LANES : (tile + 1) * LANES
                    ].astype(jnp.bfloat16)


def pack(gate, up, extra):
    pieces, deep, wide = gate.shape
    step = 8
    total = 2 * deep * wide // LANES + extra
    there = pl.BlockSpec(memory_space=pltpu.HBM)
    return pl.pallas_call(
        pack_kernel,
        in_specs=[there, there],
        out_specs=WHOLE,
        out_shape=pltpu.VMEM((pieces, total, LANES), jnp.bfloat16),
        scratch_shapes=[
            pltpu.VMEM((2, pieces // step, step, deep, wide), jnp.float32),
            pltpu.SemaphoreType.DMA((2, pieces // step)),
        ],
        compiler_params=pltpu.CompilerParams(vmem_limit_bytes=44 * 1024 * 1024),
        cost_estimate=COST,
        name="pack",
    )(gate, up)


def stamp_kernel(payload_ref, mine_ref, other_ref, gain_ref, out_ref):
    del payload_ref
    upper = lax.axis_index("owner") // 2 == 1
    mine, other = mine_ref[...] * gain_ref[...], other_ref[...] * gain_ref[...]
    both = jnp.concatenate([jnp.where(upper, other, mine), jnp.where(upper, mine, other)], axis=0).T
    half, width = both.shape[0] // 2, both.shape[1] // 2
    parts = [both[h * half : (h + 1) * half, w * width : (w + 1) * width] for w in range(2) for h in range(2)]
    swapped = jnp.concatenate([parts[i ^ 1] for i in range(4)], axis=1)
    block = jnp.where(lax.axis_index("owner") % 2 == 1, swapped, jnp.concatenate(parts, axis=1))
    block = block.astype(jnp.bfloat16)
    first = out_ref.shape[1] - half
    for piece in range(out_ref.shape[0]):
        out_ref[piece, first:, :] = block


def stamp(payload, mine, other, gain):
    return pl.pallas_call(
        stamp_kernel,
        in_specs=[WHOLE] * 4,
        out_specs=WHOLE,
        out_shape=jax.ShapeDtypeStruct(payload.shape, payload.dtype),
        input_output_aliases={0: 0},
        compiler_params=pltpu.CompilerParams(vmem_limit_bytes=16 * 1024 * 1024),
        name="stamp",
    )(payload, mine, other, gain)


def unpack_kernel(source, gate_ref, up_ref, held, sems):
    pieces = source.shape[0]
    deep = gate_ref.shape[1] // pieces
    tiles = held.shape[1]
    pair = LANES // deep

    def copy(which, tile):
        out = (gate_ref, up_ref)[which]
        return pltpu.make_async_copy(held.at[which, tile], out.at[pl.ds(tile * LANES, LANES)], sems.at[which, tile])

    @pl.loop(0, tiles)
    def _(tile):
        for which in range(2):
            start = pl.multiple_of((which * tiles + tile) * deep, deep)
            for i in range(pieces // pair):
                parts = [source[SLOT[i * pair + part], pl.ds(start, deep), :] for part in range(pair)]
                held[which, tile, :, i * LANES : (i + 1) * LANES] = jnp.concatenate(parts, axis=0).T
            copy(which, tile).start()

    @pl.loop(0, tiles)
    def _(tile):
        for which in range(2):
            copy(which, tile).wait()


def unpack(received, deep, wide):
    pieces = received.shape[0]
    there = pl.BlockSpec(memory_space=pltpu.HBM)
    shape = jax.ShapeDtypeStruct((wide, pieces * deep), jnp.bfloat16)
    return pl.pallas_call(
        unpack_kernel,
        in_specs=[WHOLE],
        out_specs=[there, there],
        out_shape=[shape, shape],
        scratch_shapes=[
            pltpu.VMEM((2, wide // LANES, LANES, pieces * deep), jnp.bfloat16),
            pltpu.SemaphoreType.DMA((2, wide // LANES)),
        ],
        compiler_params=pltpu.CompilerParams(vmem_limit_bytes=24 * 1024 * 1024),
        cost_estimate=COST,
        name="unpack",
    )(received)


def finish_kernel(mine_ref, other_ref, out_ref, held, sems):
    pieces, half, lanes = mine_ref.shape
    parts = sems.shape[0]
    step = pieces // parts
    upper = lax.axis_index("owner") % 2
    quarter = lanes // 4
    odd = lax.broadcasted_iota(jnp.int32, (step * half, lanes), 1) // quarter % 2
    own = odd == upper

    def copy(part):
        rows = pl.ds(min(MEMBERS[part * step : (part + 1) * step]), step)
        return pltpu.make_async_copy(held.at[rows], out_ref.at[rows], sems.at[part])

    for part in range(parts):
        mine = mine_ref[part * step : (part + 1) * step].reshape(step * half, lanes).astype(jnp.float32)
        other = other_ref[part * step : (part + 1) * step].reshape(step * half, lanes).astype(jnp.float32)
        crossed = jnp.where(own, other, mine)
        crossed = jnp.where(odd == 1, pltpu.roll(crossed, quarter, 1), pltpu.roll(crossed, lanes - quarter, 1))
        for h, block in enumerate((jnp.where(own, mine, other), crossed)):
            block = block.astype(jnp.bfloat16).reshape(step, half, lanes)
            for piece in range(step):
                held[MEMBERS[part * step + piece], h * half : (h + 1) * half, :] = block[piece]
        copy(part).start()
    for part in range(parts):
        copy(part).wait()


def finish(mine, other):
    pieces, half, lanes = mine.shape
    return pl.pallas_call(
        finish_kernel,
        in_specs=[WHOLE, WHOLE],
        out_specs=pl.BlockSpec(memory_space=pltpu.HBM),
        out_shape=jax.ShapeDtypeStruct((pieces, 2 * half, lanes), jnp.bfloat16),
        scratch_shapes=[pltpu.VMEM((pieces, 2 * half, lanes), jnp.bfloat16), pltpu.SemaphoreType.DMA((4,))],
        compiler_params=pltpu.CompilerParams(vmem_limit_bytes=8 * 1024 * 1024),
        name="finish",
    )(mine, other)


def on_device(train_gate, train_up, router_weight, router_gain):
    pieces, deep, wide = train_gate.shape
    part = router_weight.T
    other_part = swap(part, "yl")
    payload = pack(train_gate, train_up, deep // 2)
    body = payload.shape[1] - deep // 2
    payload = stamp(payload, part, other_part, router_gain[None, :])
    received = lax.all_to_all(
        payload, "rows", split_axis=0, concat_axis=0, axis_index_groups=[MEMBERS], tiled=True
    )
    mine = received[:, body:, :]
    other = swap(mine, "core")
    ready_gate, ready_up = unpack(received, deep, wide)
    serve_router = finish(mine, other).reshape(pieces * deep, LANES)
    return (ready_gate[None], ready_up[None], serve_router)


def solution(mesh):
    placed = (P("owner", "rows", None), P("owner", "rows", None), P("rows", "owner"), P("rows"))
    return jax.shard_map(
        on_device,
        mesh=mesh,
        in_specs=placed,
        out_specs=(P(("owner", "rows"), None, None), P(("owner", "rows"), None, None), P()),
        check_vma=False,
    )
```

```python
import jax
import jax.numpy as jnp
from jax import lax
from jax.experimental import pallas as pl
from jax.experimental.pallas import tpu as pltpu
from jax.sharding import PartitionSpec as P

AXES = ("owner", "rows")
LANES = 128
MEMBERS = [z * 8 + yh * 4 + x for z in (2, 3, 0, 1) for yh in (1, 0) for x in (2, 3, 0, 1)]
SLOT = [MEMBERS.index(row) for row in range(32)]
WHOLE = pl.BlockSpec(memory_space=pltpu.VMEM)
COST = pl.CostEstimate(flops=100_000_000, bytes_accessed=20_000_000, transcendentals=0)


def places():
    for owner in range(4):
        for row in range(32):
            yield {"z": row // 8, "yh": row // 4 % 2, "x": row % 4, "yl": owner // 2, "core": owner % 2}


def place(at):
    return (at["yl"] * 2 + at["core"]) * 32 + at["z"] * 8 + at["yh"] * 4 + at["x"]


def swap(block, axis):
    pairs = [(place(at), place(dict(at, **{axis: at[axis] ^ 1}))) for at in places()]
    return lax.ppermute(block, AXES, pairs)


def pack_kernel(gate_ref, up_ref, out_ref, held, sems):
    batches, step, deep, wide = held.shape[1:]
    tiles = wide // LANES

    def copy(which, batch):
        source = (gate_ref, up_ref)[which]
        return pltpu.make_async_copy(source.at[pl.ds(batch * step, step)], held.at[which, batch], sems.at[which, batch])

    for batch in range(batches):
        for which in range(2):
            copy(which, batch).start()

    for batch in range(batches):
        for which in range(2):
            copy(which, batch).wait()
            for piece in range(step):
                slot = SLOT[batch * step + piece]
                for tile in range(tiles):
                    first = (which * tiles + tile) * deep
                    out_ref[slot, first : first + deep, :] = held[
                        which, batch, piece, :, tile * LANES : (tile + 1) * LANES
                    ].astype(jnp.bfloat16)


def pack(gate, up, extra):
    pieces, deep, wide = gate.shape
    step = 8
    total = 2 * deep * wide // LANES + extra
    there = pl.BlockSpec(memory_space=pltpu.HBM)
    return pl.pallas_call(
        pack_kernel,
        in_specs=[there, there],
        out_specs=WHOLE,
        out_shape=pltpu.VMEM((pieces, total, LANES), jnp.bfloat16),
        scratch_shapes=[
            pltpu.VMEM((2, pieces // step, step, deep, wide), jnp.float32),
            pltpu.SemaphoreType.DMA((2, pieces // step)),
        ],
        compiler_params=pltpu.CompilerParams(vmem_limit_bytes=44 * 1024 * 1024),
        cost_estimate=COST,
        name="pack",
    )(gate, up)


def stamp_kernel(payload_ref, mine_ref, other_ref, gain_ref, out_ref):
    del payload_ref
    upper = lax.axis_index("owner") // 2 == 1
    mine, other = mine_ref[...] * gain_ref[...], other_ref[...] * gain_ref[...]
    both = jnp.concatenate([jnp.where(upper, other, mine), jnp.where(upper, mine, other)], axis=0).T
    half, width = both.shape[0] // 2, both.shape[1] // 2
    parts = [both[h * half : (h + 1) * half, w * width : (w + 1) * width] for w in range(2) for h in range(2)]
    swapped = jnp.concatenate([parts[i ^ 1] for i in range(4)], axis=1)
    block = jnp.where(lax.axis_index("owner") % 2 == 1, swapped, jnp.concatenate(parts, axis=1))
    block = block.astype(jnp.bfloat16)
    first = out_ref.shape[1] - half
    for piece in range(out_ref.shape[0]):
        out_ref[piece, first:, :] = block


def stamp(payload, mine, other, gain):
    return pl.pallas_call(
        stamp_kernel,
        in_specs=[WHOLE] * 4,
        out_specs=WHOLE,
        out_shape=jax.ShapeDtypeStruct(payload.shape, payload.dtype),
        input_output_aliases={0: 0},
        compiler_params=pltpu.CompilerParams(vmem_limit_bytes=16 * 1024 * 1024),
        name="stamp",
    )(payload, mine, other, gain)


def unpack_kernel(source, gate_ref, up_ref, held, sems):
    pieces = source.shape[0]
    deep = gate_ref.shape[1] // pieces
    tiles = held.shape[1]
    pair = LANES // deep

    def copy(which, tile):
        out = (gate_ref, up_ref)[which]
        return pltpu.make_async_copy(held.at[which, tile], out.at[pl.ds(tile * LANES, LANES)], sems.at[which, tile])

    @pl.loop(0, tiles)
    def _(tile):
        for which in range(2):
            start = pl.multiple_of((which * tiles + tile) * deep, deep)
            for i in range(pieces // pair):
                parts = [source[SLOT[i * pair + part], pl.ds(start, deep), :] for part in range(pair)]
                held[which, tile, :, i * LANES : (i + 1) * LANES] = jnp.concatenate(parts, axis=0).T
            copy(which, tile).start()

    @pl.loop(0, tiles)
    def _(tile):
        for which in range(2):
            copy(which, tile).wait()


def unpack(received, deep, wide):
    pieces = received.shape[0]
    there = pl.BlockSpec(memory_space=pltpu.HBM)
    shape = jax.ShapeDtypeStruct((wide, pieces * deep), jnp.bfloat16)
    return pl.pallas_call(
        unpack_kernel,
        in_specs=[WHOLE],
        out_specs=[there, there],
        out_shape=[shape, shape],
        scratch_shapes=[
            pltpu.VMEM((2, wide // LANES, LANES, pieces * deep), jnp.bfloat16),
            pltpu.SemaphoreType.DMA((2, wide // LANES)),
        ],
        compiler_params=pltpu.CompilerParams(vmem_limit_bytes=24 * 1024 * 1024),
        cost_estimate=COST,
        name="unpack",
    )(received)


def finish_kernel(mine_ref, other_ref, out_ref, held, sems):
    pieces, half, lanes = mine_ref.shape
    parts = sems.shape[0]
    step = pieces // parts
    upper = lax.axis_index("owner") % 2
    quarter = lanes // 4
    odd = lax.broadcasted_iota(jnp.int32, (step * half, lanes), 1) // quarter % 2
    own = odd == upper

    def copy(part):
        rows = pl.ds(min(MEMBERS[part * step : (part + 1) * step]), step)
        return pltpu.make_async_copy(held.at[rows], out_ref.at[rows], sems.at[part])

    for part in range(parts):
        mine = mine_ref[part * step : (part + 1) * step].reshape(step * half, lanes).astype(jnp.float32)
        other = other_ref[part * step : (part + 1) * step].reshape(step * half, lanes).astype(jnp.float32)
        crossed = jnp.where(own, other, mine)
        crossed = jnp.where(odd == 1, pltpu.roll(crossed, quarter, 1), pltpu.roll(crossed, lanes - quarter, 1))
        for h, block in enumerate((jnp.where(own, mine, other), crossed)):
            block = block.astype(jnp.bfloat16).reshape(step, half, lanes)
            for piece in range(step):
                held[MEMBERS[part * step + piece], h * half : (h + 1) * half, :] = block[piece]
        copy(part).start()
    for part in range(parts):
        copy(part).wait()


def finish(mine, other):
    pieces, half, lanes = mine.shape
    return pl.pallas_call(
        finish_kernel,
        in_specs=[WHOLE, WHOLE],
        out_specs=pl.BlockSpec(memory_space=pltpu.HBM),
        out_shape=jax.ShapeDtypeStruct((pieces, 2 * half, lanes), jnp.bfloat16),
        scratch_shapes=[pltpu.VMEM((pieces, 2 * half, lanes), jnp.bfloat16), pltpu.SemaphoreType.DMA((4,))],
        compiler_params=pltpu.CompilerParams(vmem_limit_bytes=8 * 1024 * 1024),
        name="finish",
    )(mine, other)


def on_device(train_gate, train_up, router_weight, router_gain):
    pieces, deep, wide = train_gate.shape
    part = router_weight.T
    other_part = swap(part, "yl")
    payload = pack(train_gate, train_up, deep // 2)
    body = payload.shape[1] - deep // 2
    payload = stamp(payload, part, other_part, router_gain[None, :])
    received = lax.all_to_all(
        payload, "rows", split_axis=0, concat_axis=0, axis_index_groups=[MEMBERS], tiled=True
    )
    mine = received[:, body:, :]
    other = swap(mine, "core")
    ready_gate, ready_up = unpack(received, deep, wide)
    serve_router = finish(mine, other).reshape(pieces * deep, LANES)
    return (ready_gate[None], ready_up[None], serve_router)


def solution(mesh):
    placed = (P("owner", "rows", None), P("owner", "rows", None), P("rows", "owner"), P("rows"))
    return jax.shard_map(
        on_device,
        mesh=mesh,
        in_specs=placed,
        out_specs=(P(("owner", "rows"), None, None), P(("owner", "rows"), None, None), P()),
        check_vma=False,
    )
```

```python
import jax
import jax.numpy as jnp
from jax import lax
from jax.experimental import pallas as pl
from jax.experimental.pallas import tpu as pltpu
from jax.sharding import PartitionSpec as P

AXES = ("owner", "rows")
LANES = 128
MEMBERS = [z * 8 + yh * 4 + x for z in (2, 3, 0, 1) for yh in (1, 0) for x in (2, 3, 0, 1)]
SLOT = [MEMBERS.index(row) for row in range(32)]
WHOLE = pl.BlockSpec(memory_space=pltpu.VMEM)
COST = pl.CostEstimate(flops=100_000_000, bytes_accessed=20_000_000, transcendentals=0)


def places():
    for owner in range(4):
        for row in range(32):
            yield {"z": row // 8, "yh": row // 4 % 2, "x": row % 4, "yl": owner // 2, "core": owner % 2}


def place(at):
    return (at["yl"] * 2 + at["core"]) * 32 + at["z"] * 8 + at["yh"] * 4 + at["x"]


def swap(block, axis):
    pairs = [(place(at), place(dict(at, **{axis: at[axis] ^ 1}))) for at in places()]
    return lax.ppermute(block, AXES, pairs)


def pack_kernel(gate_ref, up_ref, out_ref, held, sems):
    batches, step, deep, wide = held.shape[1:]
    tiles = wide // LANES

    def copy(which, batch):
        source = (gate_ref, up_ref)[which]
        return pltpu.make_async_copy(source.at[pl.ds(batch * step, step)], held.at[which, batch], sems.at[which, batch])

    for batch in range(batches):
        for which in range(2):
            copy(which, batch).start()

    for batch in range(batches):
        for which in range(2):
            copy(which, batch).wait()
            for piece in range(step):
                slot = SLOT[batch * step + piece]
                for tile in range(tiles):
                    first = (which * tiles + tile) * deep
                    out_ref[slot, first : first + deep, :] = held[
                        which, batch, piece, :, tile * LANES : (tile + 1) * LANES
                    ].astype(jnp.bfloat16)


def pack(gate, up, extra):
    pieces, deep, wide = gate.shape
    step = 8
    total = 2 * deep * wide // LANES + extra
    there = pl.BlockSpec(memory_space=pltpu.HBM)
    return pl.pallas_call(
        pack_kernel,
        in_specs=[there, there],
        out_specs=WHOLE,
        out_shape=pltpu.VMEM((pieces, total, LANES), jnp.bfloat16),
        scratch_shapes=[
            pltpu.VMEM((2, pieces // step, step, deep, wide), jnp.float32),
            pltpu.SemaphoreType.DMA((2, pieces // step)),
        ],
        compiler_params=pltpu.CompilerParams(vmem_limit_bytes=44 * 1024 * 1024),
        cost_estimate=COST,
        name="pack",
    )(gate, up)


def stamp_kernel(payload_ref, mine_ref, other_ref, gain_ref, out_ref):
    del payload_ref
    upper = lax.axis_index("owner") // 2 == 1
    mine, other = mine_ref[...] * gain_ref[...], other_ref[...] * gain_ref[...]
    both = jnp.concatenate([jnp.where(upper, other, mine), jnp.where(upper, mine, other)], axis=0).T
    half, width = both.shape[0] // 2, both.shape[1] // 2
    parts = [both[h * half : (h + 1) * half, w * width : (w + 1) * width] for w in range(2) for h in range(2)]
    swapped = jnp.concatenate([parts[i ^ 1] for i in range(4)], axis=1)
    block = jnp.where(lax.axis_index("owner") % 2 == 1, swapped, jnp.concatenate(parts, axis=1))
    block = block.astype(jnp.bfloat16)
    first = out_ref.shape[1] - half
    for piece in range(out_ref.shape[0]):
        out_ref[piece, first:, :] = block


def stamp(payload, mine, other, gain):
    return pl.pallas_call(
        stamp_kernel,
        in_specs=[WHOLE] * 4,
        out_specs=WHOLE,
        out_shape=jax.ShapeDtypeStruct(payload.shape, payload.dtype),
        input_output_aliases={0: 0},
        compiler_params=pltpu.CompilerParams(vmem_limit_bytes=16 * 1024 * 1024),
        name="stamp",
    )(payload, mine, other, gain)


def unpack_kernel(source, gate_ref, up_ref, held, sems):
    pieces = source.shape[0]
    deep = gate_ref.shape[1] // pieces
    tiles = held.shape[1]
    pair = LANES // deep

    groups = pieces // pair
    width = groups // 2 * LANES

    def copy(which, tile, half):
        out = (gate_ref, up_ref)[which].at[pl.ds(tile * LANES, LANES), pl.ds(half * width, width)]
        return pltpu.make_async_copy(held.at[which, tile, :, pl.ds(half * width, width)], out, sems.at[which, tile, half])

    @pl.loop(0, tiles)
    def _(tile):
        for which in range(2):
            start = pl.multiple_of((which * tiles + tile) * deep, deep)
            for i in range(pieces // pair):
                parts = [source[SLOT[i * pair + part], pl.ds(start, deep), :] for part in range(pair)]
                held[which, tile, :, i * LANES : (i + 1) * LANES] = jnp.concatenate(parts, axis=0).T
                if i % (groups // 2) == groups // 2 - 1:
                    copy(which, tile, i // (groups // 2)).start()

    @pl.loop(0, tiles)
    def _(tile):
        for which in range(2):
            for half in range(2):
                copy(which, tile, half).wait()


def unpack(received, deep, wide):
    pieces = received.shape[0]
    there = pl.BlockSpec(memory_space=pltpu.HBM)
    shape = jax.ShapeDtypeStruct((wide, pieces * deep), jnp.bfloat16)
    return pl.pallas_call(
        unpack_kernel,
        in_specs=[WHOLE],
        out_specs=[there, there],
        out_shape=[shape, shape],
        scratch_shapes=[
            pltpu.VMEM((2, wide // LANES, LANES, pieces * deep), jnp.bfloat16),
            pltpu.SemaphoreType.DMA((2, wide // LANES, 2)),
        ],
        compiler_params=pltpu.CompilerParams(vmem_limit_bytes=24 * 1024 * 1024),
        cost_estimate=COST,
        name="unpack",
    )(received)


def finish_kernel(mine_ref, other_ref, out_ref, held, sems):
    pieces, half, lanes = mine_ref.shape
    parts = sems.shape[0]
    step = pieces // parts
    upper = lax.axis_index("owner") % 2
    quarter = lanes // 4
    odd = lax.broadcasted_iota(jnp.int32, (step * half, lanes), 1) // quarter % 2
    own = odd == upper

    def copy(part):
        rows = pl.ds(min(MEMBERS[part * step : (part + 1) * step]), step)
        return pltpu.make_async_copy(held.at[rows], out_ref.at[rows], sems.at[part])

    for part in range(parts):
        mine = mine_ref[part * step : (part + 1) * step].reshape(step * half, lanes).astype(jnp.float32)
        other = other_ref[part * step : (part + 1) * step].reshape(step * half, lanes).astype(jnp.float32)
        crossed = jnp.where(own, other, mine)
        crossed = jnp.where(odd == 1, pltpu.roll(crossed, quarter, 1), pltpu.roll(crossed, lanes - quarter, 1))
        for h, block in enumerate((jnp.where(own, mine, other), crossed)):
            block = block.astype(jnp.bfloat16).reshape(step, half, lanes)
            for piece in range(step):
                held[MEMBERS[part * step + piece], h * half : (h + 1) * half, :] = block[piece]
        copy(part).start()
    for part in range(parts):
        copy(part).wait()


def finish(mine, other):
    pieces, half, lanes = mine.shape
    return pl.pallas_call(
        finish_kernel,
        in_specs=[WHOLE, WHOLE],
        out_specs=pl.BlockSpec(memory_space=pltpu.HBM),
        out_shape=jax.ShapeDtypeStruct((pieces, 2 * half, lanes), jnp.bfloat16),
        scratch_shapes=[pltpu.VMEM((pieces, 2 * half, lanes), jnp.bfloat16), pltpu.SemaphoreType.DMA((4,))],
        compiler_params=pltpu.CompilerParams(vmem_limit_bytes=8 * 1024 * 1024),
        name="finish",
    )(mine, other)


def on_device(train_gate, train_up, router_weight, router_gain):
    pieces, deep, wide = train_gate.shape
    part = router_weight.T
    other_part = swap(part, "yl")
    payload = pack(train_gate, train_up, deep // 2)
    body = payload.shape[1] - deep // 2
    payload = stamp(payload, part, other_part, router_gain[None, :])
    received = lax.all_to_all(
        payload, "rows", split_axis=0, concat_axis=0, axis_index_groups=[MEMBERS], tiled=True
    )
    mine = received[:, body:, :]
    other = swap(mine, "core")
    ready_gate, ready_up = unpack(received, deep, wide)
    serve_router = finish(mine, other).reshape(pieces * deep, LANES)
    return (ready_gate[None], ready_up[None], serve_router)


def solution(mesh):
    placed = (P("owner", "rows", None), P("owner", "rows", None), P("rows", "owner"), P("rows"))
    return jax.shard_map(
        on_device,
        mesh=mesh,
        in_specs=placed,
        out_specs=(P(("owner", "rows"), None, None), P(("owner", "rows"), None, None), P()),
        check_vma=False,
    )
```
